32 devices in a mesh: tok: 4 (over y, core), cache: 8 (over z, x).
Axes of the slice: x: 2, y: 2, z: 4, core: 2. Of those that a mesh axis runs over, the one named last changes fastest.
Arguments:
- queries_one: bfloat16 [64, 6, 128, 576], P('cache', None, 'tok'), may hold values from -100 to 100
- keys_one: bfloat16 [64, 6, 576], P('cache'), may hold values from -12 to 12
- queries_two: bfloat16 [64, 6, 128, 576], P('cache', None, 'tok'), may hold values from -100 to 100
- keys_two: bfloat16 [64, 6, 576], P('cache'), may hold values from -12 to 12
- latent_cache: bfloat16 [64, 640, 576], P('cache'), may hold values from -8 to 8
- cached_len: int32 [64], P('cache'), may hold values from 80 to 640
- first_owner: int32 [64], P('cache'), may hold values from 0 to 7, as said below
- new_owner: int32 [64], P('cache'), may hold values from 0 to 7, as said below
- accepted: int32 [64], P('cache'), may hold values from 1 to 6
Outputs:
- first_out: bfloat16 [64, 6, 128, 512], P('cache', None, 'tok')
- second_out: bfloat16 [64, 6, 128, 512], P('cache', None, 'tok')
- arrived_cache: bfloat16 [32, 640, 576], P('cache')
The draws below stay inside these ranges and needn't reach their ends.
Inputs may be any that keep to these rules, and one draw needn't show every extreme that they name: `first_owner`: row j of a device's 8 draft rows is the request whose cache lies in slot j of the named cache device in round one; the rows of one device name every cache device exactly once, and every slot is named by exactly one row. `new_owner`: each slot's cache keeps its position j in round two. On every device the same half of the positions j name another device and the rest the device itself; the other devices that one device names are distinct, and every device receives exactly one cache into each slot that it gives up. The round-two devices of one device's draft rows name no cache device more than 2 times, and on every device some cache device exactly 2 times.
All inputs are finite; a program needn't handle non-finite values.
Results may differ from the reference program's by a relative error of at most 0.0032.
Values may be sent and summed in bfloat16 or wider, within the bound.
No kernel may reach another device: no remote copies, remote signals or barrier semaphores. Data moves between devices by JAX's collectives and lax.ppermute only.
A program may use at most 128 MiB of HBM per device.

```python
import jax
import jax.numpy as jnp
from jax import lax

H = 128
LAT = 512
ROPE = 64
DRAFT = 6
CTX = 640
REQS = 64
N_CACHE = 8


def layout_tables(key):
    peer_count = N_CACHE
    half_count = peer_count // 2
    base_key = jax.random.fold_in(key, 7001)
    key_one, key_two, key_three = jax.random.split(base_key, 3)
    relabel = jax.random.permutation(key_one, peer_count).astype(jnp.int32)
    high_bits = jax.random.randint(key_two, (half_count,), 0, 2).astype(jnp.int32)
    high_bits = high_bits.at[0].set(1)
    residues = jnp.arange(half_count, dtype=jnp.int32)
    mover_start = residues + half_count * high_bits
    stayer_start = residues + half_count * (1 - high_bits)
    mover_end = 2 * residues
    column_order = jax.random.permutation(key_three, peer_count).astype(jnp.int32)
    offset_one = jnp.zeros((peer_count,), jnp.int32).at[column_order].set(jnp.concatenate([mover_start, stayer_start]))
    offset_two = jnp.zeros((peer_count,), jnp.int32).at[column_order].set(jnp.concatenate([mover_end, stayer_start]))
    drafters = jnp.arange(peer_count, dtype=jnp.int32)
    first_table = relabel[(drafters[:, None] + offset_one[None, :]) % peer_count]
    second_table = relabel[(drafters[:, None] + offset_two[None, :]) % peer_count]
    return (first_table, second_table)


def draw_first_owner(key, part):
    first_table, second_table = layout_tables(key)
    return first_table.reshape(-1)


def draw_new_owner(key, part):
    first_table, second_table = layout_tables(key)
    peer_count = N_CACHE
    column_ids = jnp.broadcast_to(jnp.arange(peer_count, dtype=jnp.int32)[None, :], (peer_count, peer_count))
    settled = jnp.zeros((peer_count, peer_count), jnp.int32).at[first_table, column_ids].set(second_table)
    return settled.reshape(-1)


def cache_values(key):
    inner_key = jax.random.fold_in(key, 7002)
    values = jnp.clip(jax.random.normal(inner_key, (REQS, CTX, LAT + ROPE), jnp.float32), -6.0, 6.0)
    return values.astype(jnp.bfloat16)


def draw_latent_cache(key, part):
    return cache_values(key)


def drawn_queries(key, salt):
    inner_key = jax.random.fold_in(key, salt)
    values = jnp.clip(jax.random.normal(inner_key, (REQS, DRAFT, H, LAT + ROPE), jnp.float32), -6.0, 6.0)
    return values.astype(jnp.bfloat16)


def draw_queries_one(key, part):
    return drawn_queries(key, 7003)


def draw_queries_two(key, part):
    return drawn_queries(key, 7004)


def set_ends(values, key, low, high):
    index_at = [jax.random.randint(jax.random.fold_in(key, axis), (), 0, length) for axis, length in enumerate(values.shape)]
    widest = values.shape.index(max(values.shape))
    next_to = index_at[:widest] + [(index_at[widest] + 1) % values.shape[widest]] + index_at[widest + 1:]
    return values.at[tuple(index_at)].set(low).at[tuple(next_to)].set(high)


def steps_of(rng, dims, shards, smallest, largest):
    def one(position, parts):
        draws = jax.random.uniform(jax.random.fold_in(jax.random.fold_in(rng, 6), position), (parts,), jnp.float32, smallest / len(shards), largest / len(shards))
        return jnp.repeat(jnp.exp(draws), dims[position] // parts).reshape((-1,) + (1,) * (len(dims) - position - 1))

    level = one(*shards[0])
    for cut in shards[1:]:
        level = level * one(*cut)
    return level


def noise(rng, dims, deviation, reach, cuts=(), kind=jnp.bfloat16):
    gain = steps_of(rng, dims, cuts, -0.22, 0.18) if cuts else 1.0
    values = jax.random.normal(rng, dims, jnp.float32) * deviation * gain
    return jnp.minimum(jnp.maximum(values, -reach), reach).astype(kind)


def setup_inputs(seed: int = 0) -> dict:
    key_of = jax.random.split(jax.random.key(seed), 10)
    queries_one = draw_queries_one(jax.random.fold_in(key_of[9], 71), 0)
    keys_one = noise(key_of[1], (REQS, DRAFT, LAT + ROPE), 2.0, 12.0, ((0, 8),))
    queries_two = draw_queries_two(jax.random.fold_in(key_of[9], 71), 0)
    keys_two = noise(key_of[3], (REQS, DRAFT, LAT + ROPE), 2.0, 12.0, ((0, 8),))
    latent_cache = draw_latent_cache(jax.random.fold_in(key_of[9], 71), 0)
    cached_len = set_ends(jax.random.randint(key_of[5], (REQS,), CTX // 8, CTX + 1), jax.random.fold_in(key_of[5], 1), CTX // 8, CTX).astype(jnp.int32)
    first_owner = draw_first_owner(jax.random.fold_in(key_of[9], 71), 0)
    new_owner = draw_new_owner(jax.random.fold_in(key_of[9], 71), 0)
    accepted = set_ends(jax.random.randint(key_of[8], (REQS,), 1, DRAFT + 1), jax.random.fold_in(key_of[8], 1), 1, DRAFT).astype(jnp.int32)
    return dict(queries_one=queries_one, keys_one=keys_one, queries_two=queries_two, keys_two=keys_two, latent_cache=latent_cache, cached_len=cached_len, first_owner=first_owner, new_owner=new_owner, accepted=accepted)


score_factor = 192.0 ** -0.5


def attend(queries, cache_rows, length, extra_keys, extra_mask):
    query_wide = queries.astype(jnp.float32)
    cache_wide = cache_rows.astype(jnp.float32)
    extra_wide = extra_keys.astype(jnp.float32)
    near_score = jnp.einsum("rhw,cw->rhc", query_wide, cache_wide) * score_factor
    places = jnp.arange(cache_rows.shape[0], dtype=jnp.int32)
    near_score = jnp.where((places < length)[None, None, :], near_score, -jnp.inf)
    own_score = jnp.einsum("rhw,ew->rhe", query_wide, extra_wide) * score_factor
    own_score = jnp.where(extra_mask[:, None, :], own_score, -jnp.inf)
    row_max = jnp.maximum(jnp.max(near_score, axis=-1), jnp.max(own_score, axis=-1))
    near_weight = jnp.exp(near_score - row_max[..., None])
    own_weight = jnp.exp(own_score - row_max[..., None])
    denominator = jnp.sum(near_weight, axis=-1) + jnp.sum(own_weight, axis=-1)
    near_round = lax.optimization_barrier(near_weight.astype(jnp.bfloat16)).astype(jnp.float32)
    own_round = lax.optimization_barrier(own_weight.astype(jnp.bfloat16)).astype(jnp.float32)
    mixture = jnp.einsum("rhc,cl->rhl", near_round, cache_wide[:, :LAT])
    mixture = mixture + jnp.einsum("rhe,el->rhl", own_round, extra_wide[:, :LAT])
    return (mixture / denominator[..., None]).astype(jnp.bfloat16)


def reference(queries_one, keys_one, queries_two, keys_two, latent_cache, cached_len, first_owner, new_owner, accepted):
    peer_count = N_CACHE
    column_ids = (jnp.arange(REQS, dtype=jnp.int32) % peer_count).astype(jnp.int32)
    slot_one = (first_owner * peer_count + column_ids).astype(jnp.int32)
    row_ids = jnp.arange(DRAFT, dtype=jnp.int32)
    causal = row_ids[:, None] >= row_ids[None, :]

    def one_request(request):
        slot = slot_one[request]
        cache_rows = lax.dynamic_index_in_dim(latent_cache, slot, 0, keepdims=False)
        length = cached_len[slot]
        first_rows = attend(queries_one[request], cache_rows, length, keys_one[request], causal)
        both_keys = jnp.concatenate([keys_one[request], keys_two[request]], axis=0)
        kept_rows = jnp.broadcast_to((row_ids < accepted[request])[None, :], (DRAFT, DRAFT))
        mask_two = jnp.concatenate([kept_rows, causal], axis=1)
        second_rows = attend(queries_two[request], cache_rows, length, both_keys, mask_two)
        return first_rows, second_rows

    first_out, second_out = lax.map(one_request, jnp.arange(REQS, dtype=jnp.int32))
    target = (new_owner * peer_count + column_ids).astype(jnp.int32)
    source = jnp.zeros((REQS,), jnp.int32).at[target].set(jnp.arange(REQS, dtype=jnp.int32))
    moved_cols = jnp.nonzero(new_owner[:peer_count] != 0, size=peer_count // 2)[0].astype(jnp.int32)
    arrived_ids = source.reshape(peer_count, peer_count)[:, moved_cols].reshape(-1).astype(jnp.int32)
    arrived_cache = jnp.take(latent_cache, arrived_ids, axis=0)
    return first_out, second_out, arrived_cache
```

```python
import functools

import jax
import jax.numpy as jnp
from jax import lax
from jax.experimental import pallas as pl
from jax.experimental.pallas import tpu as pltpu
from jax.sharding import PartitionSpec as P

LAT = 512
CORES = 2
ROWS = 16

score_factor = 192.0 ** (-0.5)
log2_e = 1.4426950408889634
ANY = pl.BlockSpec(memory_space=pl.ANY)
SMEM = pl.BlockSpec(memory_space=pltpu.SMEM)
VMEM = pl.BlockSpec(memory_space=pltpu.VMEM)


def round_up(value, step):
    return -(-value // step) * step


def take_kernel(count, pick_ref, base_ref, table_ref, out_ref, sems):
    rows = out_ref.shape[1]
    base = pl.multiple_of(base_ref[0], ROWS)
    copies = [
        pltpu.make_async_copy(
            table_ref.at[pick_ref[d], pl.ds(base, rows)], out_ref.at[d], sems.at[d]
        )
        for d in range(count)
    ]
    for copy in copies:
        copy.start()
    for copy in copies:
        copy.wait()


def take_rows(table, pick, base, rows):
    count = pick.shape[0]
    size = count * rows * table.shape[2] * table.dtype.itemsize
    return pl.pallas_call(
        functools.partial(take_kernel, count),
        out_shape=jax.ShapeDtypeStruct((count, rows, table.shape[2]), table.dtype),
        in_specs=[SMEM, SMEM, ANY],
        out_specs=VMEM,
        scratch_shapes=[pltpu.SemaphoreType.DMA((count,))],
        cost_estimate=pl.CostEstimate(flops=2 * size, bytes_accessed=2 * size, transcendentals=0),
        name="take_rows",
    )(pick, base[None], table)


def place_kernel(spans, count, starts_ref, *refs):
    parts, out_ref, bufs = refs[: len(spans)], refs[len(spans)], refs[len(spans) + 1 : -2]
    in_sems, out_sems = refs[-2:]
    loads, stores = [], []
    for p, (origin, off, rows) in enumerate(spans):
        base = pl.multiple_of(starts_ref[origin] + off, ROWS)
        for k in range(count):
            loads.append(
                pltpu.make_async_copy(parts[p].at[k], bufs[p].at[k], in_sems.at[p, k])
            )
            stores.append(
                pltpu.make_async_copy(
                    bufs[p].at[k], out_ref.at[k, pl.ds(base, rows)], out_sems.at[p, k]
                )
            )
    for load in loads:
        load.start()
    for load, store in zip(loads, stores):
        load.wait()
        store.start()
    for store in stores:
        store.wait()


def place_parts(parts, spans, starts, width):
    count, _, lanes = parts[0].shape
    dtype = parts[0].dtype
    size = count * width * lanes * dtype.itemsize
    return pl.pallas_call(
        functools.partial(place_kernel, spans, count),
        out_shape=jax.ShapeDtypeStruct((count, width, lanes), dtype),
        in_specs=[SMEM] + [ANY] * len(parts),
        out_specs=ANY,
        scratch_shapes=[pltpu.VMEM(part.shape, dtype) for part in parts]
        + [pltpu.SemaphoreType.DMA((len(parts), count))] * 2,
        cost_estimate=pl.CostEstimate(flops=2 * size, bytes_accessed=2 * size, transcendentals=0),
        name="place_parts",
    )(starts, *parts)


def attend(queries, keys_t, length, extra, extra_mask):
    scale = score_factor * log2_e
    near = jnp.dot(queries, keys_t, preferred_element_type=jnp.float32) * scale
    places = lax.broadcasted_iota(jnp.int32, (1, keys_t.shape[1]), 1)
    near = jnp.where(places < length, near, -jnp.inf)
    own = (
        lax.dot_general(
            queries, extra, (((1,), (1,)), ((), ())), preferred_element_type=jnp.float32
        )
        * scale
    )
    own = jnp.where(extra_mask, own, -jnp.inf)
    row_max = jnp.maximum(
        jnp.max(near, axis=1, keepdims=True), jnp.max(own, axis=1, keepdims=True)
    )
    near_weight = jnp.exp2(near - row_max)
    own_weight = jnp.exp2(own - row_max)
    total = jnp.sum(near_weight, axis=1, keepdims=True) + jnp.sum(
        own_weight, axis=1, keepdims=True
    )
    mixture = lax.dot_general(
        near_weight.astype(jnp.bfloat16),
        keys_t[:LAT],
        (((1,), (1,)), ((), ())),
        preferred_element_type=jnp.float32,
    )
    mixture = mixture + jnp.dot(
        own_weight.astype(jnp.bfloat16), extra[:, :LAT], preferred_element_type=jnp.float32
    )
    return (mixture * (1.0 / total)).astype(jnp.bfloat16)


def attend_kernel(spans, draft, owner_ref, length_ref, accept_ref, starts_ref, *refs):
    q1_ref, q2_ref, extra_ref = refs[:3]
    parts = refs[3 : 3 + len(spans)]
    o1_ref, o2_ref, held, sems = refs[3 + len(spans) :]
    step, steps = pl.program_id(0), pl.num_programs(0)

    def copies(r):
        for p, (origin, off, rows) in enumerate(spans):
            base = pl.multiple_of(starts_ref[origin] + off, ROWS)
            yield pltpu.make_async_copy(
                parts[p].at[owner_ref[r]], held.at[r, pl.ds(base, rows)], sems.at[r, p]
            )

    @pl.when(step == 0)
    def _():
        @pl.loop(0, steps)
        def _(r):
            for copy in copies(r):
                copy.start()

    for copy in copies(step):
        copy.wait()
    rows = q1_ref.shape[1]
    heads = rows // draft
    extra = extra_ref[0]
    row = lax.broadcasted_iota(jnp.int32, (rows, extra.shape[0]), 0)
    col = lax.broadcasted_iota(jnp.int32, (rows, extra.shape[0]), 1)
    causal_one = (col < draft) & (row >= col * heads)
    causal_two = (col >= draft) & (col < 2 * draft) & (row >= (col - draft) * heads)
    kept = (col < draft) & (col < accept_ref[step])
    keys_t = held[step]
    length = length_ref[step]
    o1_ref[0] = attend(q1_ref[0], keys_t, length, extra, causal_one)
    o2_ref[0] = attend(q2_ref[0], keys_t, length, extra, kept | causal_two)


def attend_all(q1, q2, extra, parts, spans, starts, owner, length, accepted, draft):
    reqs, rows, width = q1.shape
    positions = parts[0].shape[2]
    pieces = len(parts)
    block = lambda lanes: pl.BlockSpec((1, rows, lanes), lambda r: (r, 0, 0))
    out = jax.ShapeDtypeStruct((reqs, rows, LAT), jnp.bfloat16)
    flops = 2 * 2 * reqs * rows * positions * (width + LAT)
    return pl.pallas_call(
        functools.partial(attend_kernel, spans, draft),
        grid=(reqs,),
        out_shape=(out, out),
        in_specs=[SMEM] * 4
        + [block(width), block(width)]
        + [pl.BlockSpec((1,) + extra.shape[1:], lambda r: (r, 0, 0))]
        + [ANY] * pieces,
        out_specs=(block(LAT), block(LAT)),
        scratch_shapes=[
            pltpu.VMEM((reqs, width, positions), jnp.bfloat16),
            pltpu.SemaphoreType.DMA((reqs, pieces)),
        ],
        cost_estimate=pl.CostEstimate(
            flops=flops, bytes_accessed=reqs * width * positions * 4, transcendentals=0
        ),
        compiler_params=pltpu.CompilerParams(dimension_semantics=("arbitrary",)),
        name="attend_all",
    )(owner, length, accepted, starts, q1, q2, extra, *parts)


def local(
    queries_one,
    keys_one,
    queries_two,
    keys_two,
    latent_cache,
    cached_len,
    first_owner,
    new_owner,
    accepted,
):
    peers = lax.axis_size("cache")
    me = lax.axis_index("cache")
    groups = lax.axis_size("tok")
    group = lax.axis_index("tok")
    chips = groups // CORES
    reqs, draft, heads, width = queries_one.shape
    columns = jnp.arange(peers, dtype=jnp.int32)

    def pick(table, hits, axis):
        return jnp.sum(jnp.where(hits, table, 0), axis=axis, dtype=jnp.int32)

    def exchange(x):
        return lax.all_to_all(x, "cache", split_axis=0, concat_axis=0, tiled=True)

    owned = first_owner[None, :] == columns[:, None]
    pick_one = pick(columns[None, :], owned, 1)
    told = jnp.concatenate(
        [
            pick_one[:, None],
            jnp.broadcast_to(cached_len[None, :], (peers, reqs)),
            jnp.broadcast_to(new_owner[None, :], (peers, reqs)),
        ],
        axis=1,
    )
    heard = exchange(told)
    sent_slot = heard[:, 0]
    all_len = heard[:, 1 : 1 + reqs]
    all_new = heard[:, 1 + reqs :]
    length = pick(all_len, owned, 0)

    cache_t = jnp.swapaxes(latent_cache, 1, 2)
    share = round_up(-(-width // groups), ROWS)
    start_of = lambda t: jnp.minimum(t * share, width - share).astype(jnp.int32)
    base = start_of(group)
    chip, core = group // CORES, group % CORES
    origins = [group] + [(chip + chips - s) % chips * CORES + core for s in range(1, chips)]
    origins += [t + 1 - 2 * core for t in origins]
    starts = jnp.stack([start_of(t) for t in origins])

    def spread(part):
        held = [part]
        for s in range(1, chips):
            hop = [
                (c * CORES + k, (c + s) % chips * CORES + k)
                for c in range(chips)
                for k in range(CORES)
            ]
            held.append(lax.ppermute(part, "tok", hop))
        swap = [(t, t + 1 - 2 * (t % CORES)) for t in range(groups)]
        return held + [lax.ppermute(x, "tok", swap) for x in held]

    def cuts(count):
        size = round_up(-(-share // count), ROWS)
        return [(off, min(size, share - off)) for off in range(0, share, size)]

    draft_parts, draft_spans = [], []
    for off, rows in cuts(1):
        came = exchange(take_rows(cache_t, sent_slot, base + off, rows))
        draft_parts += spread(came)
        draft_spans += [(k, off, rows) for k in range(groups)]

    moving = new_owner != me
    sent_move = pick(columns[None, :], (new_owner[None, :] == columns[:, None]) & moving[None, :], 1)
    source = pick(columns[:, None], all_new == me, 0)
    order = jnp.cumsum(moving.astype(jnp.int32)) - 1
    moved = jnp.arange(peers // 2, dtype=jnp.int32)
    moved_source = pick(source[None, :], (order[None, :] == moved[:, None]) & moving[None, :], 1)
    move_parts, move_spans = [], []
    for off, rows in cuts(1):
        came = exchange(take_rows(cache_t, sent_move, base + off, rows))
        real = take_rows(came, moved_source, jnp.int32(0), rows)
        move_parts += spread(real)
        move_spans += [(k, off, rows) for k in range(groups)]
    arrived = place_parts(move_parts, move_spans, starts, width)

    extra = jnp.concatenate([keys_one, keys_two], axis=1)
    extra = jnp.pad(extra, ((0, 0), (0, round_up(2 * draft, ROWS) - 2 * draft), (0, 0)))
    flat = (reqs, draft * heads, width)
    first_out, second_out = attend_all(
        queries_one.reshape(flat),
        queries_two.reshape(flat),
        extra,
        draft_parts,
        draft_spans,
        starts,
        first_owner,
        length,
        accepted,
        draft,
    )
    shape = (reqs, draft, heads, LAT)
    return first_out.reshape(shape), second_out.reshape(shape), jnp.swapaxes(arrived, 1, 2)


def solution(mesh):
    placed = (
        P("cache", None, "tok", None),
        P("cache", None, None),
        P("cache", None, "tok", None),
        P("cache", None, None),
        P("cache", None, None),
        P("cache"),
        P("cache"),
        P("cache"),
        P("cache"),
    )
    return jax.shard_map(
        local,
        mesh=mesh,
        in_specs=placed,
        out_specs=(
            P("cache", None, "tok", None),
            P("cache", None, "tok", None),
            P("cache", None, None),
        ),
        check_vma=False,
    )
```

```python
import functools

import jax
import jax.numpy as jnp
from jax import lax
from jax.experimental import pallas as pl
from jax.experimental.pallas import tpu as pltpu
from jax.sharding import PartitionSpec as P


LAT = 512
CORES = 2
ROWS = 16

score_factor = 192.0 ** (-0.5)
log2_e = 1.4426950408889634
ANY = pl.BlockSpec(memory_space=pl.ANY)
SMEM = pl.BlockSpec(memory_space=pltpu.SMEM)
VMEM = pl.BlockSpec(memory_space=pltpu.VMEM)


def round_up(value, step):
    return -(-value // step) * step


def tell_kernel(first_ref, length_ref, move_ref, out_ref):
    reqs = first_ref.shape[0]
    lane = lax.broadcasted_iota(jnp.int32, out_ref.shape, 1)
    row = jnp.zeros(out_ref.shape, jnp.int32)
    for t, ref in enumerate((first_ref, length_ref, move_ref)):
        for j in range(reqs):
            row = jnp.where(lane == t * reqs + j, ref[j], row)
    out_ref[...] = row


def tell(first_owner, cached_len, new_owner, peers):
    return pl.pallas_call(
        tell_kernel,
        out_shape=jax.ShapeDtypeStruct((peers, 3 * first_owner.shape[0]), jnp.int32),
        in_specs=[SMEM] * 3,
        out_specs=VMEM,
        name="tell",
    )(first_owner, cached_len, new_owner)


def peer_of(me, half, s, to):
    side, place = me // half, me % half
    if s < half:
        return side * half + s
    shift = s - half if to else 2 * half - s
    return (1 - side) * half + lax.rem(place + shift, half)


def take_kernel(plan, half, moves, meta_ref, slots_ref, table_ref, *refs):
    outs, sems = refs[: len(plan)], refs[len(plan)]
    me = meta_ref[0]
    copies = []
    for out_ref, (first, part) in zip(outs, plan):
        base = pl.multiple_of(meta_ref[part], ROWS)
        for d in range(out_ref.shape[0]):
            peer = peer_of(me, half, first + d, True)
            slot = jnp.int32(0)
            for j in range(2 * half):
                if moves:
                    hit = (slots_ref[j] == peer) & (peer != me)
                else:
                    hit = slots_ref[peer, j] == me
                slot = jnp.where(hit, j, slot)
            copies.append(
                pltpu.make_async_copy(
                    table_ref.at[slot, pl.ds(base, out_ref.shape[1])],
                    out_ref.at[d],
                    sems.at[first + d],
                )
            )
    for copy in copies:
        copy.start()
    for copy in copies:
        copy.wait()


def take_rows(table, meta, slots, moves, plan, shapes):
    lanes = table.shape[2]
    count = sum(shape[0] for shape in shapes)
    size = sum(n * rows for n, rows in shapes) * lanes * table.dtype.itemsize
    return pl.pallas_call(
        functools.partial(take_kernel, plan, count // 2, moves),
        out_shape=[jax.ShapeDtypeStruct(shape + (lanes,), table.dtype) for shape in shapes],
        in_specs=[SMEM, SMEM, ANY],
        out_specs=[VMEM] * len(shapes),
        scratch_shapes=[pltpu.SemaphoreType.DMA((count,))],
        cost_estimate=pl.CostEstimate(flops=2 * size, bytes_accessed=2 * size, transcendentals=0),
        name="take_rows",
    )(meta, slots, table)


def place_kernel(groups, kept, half, meta_ref, heard_ref, move_ref, *refs):
    count = len(groups)
    reqs = move_ref.shape[0]
    me = meta_ref[0]
    order, leaves = [], []
    rank = jnp.int32(0)
    for j in range(reqs):
        leaves.append(move_ref[j] != me)
        order.append(rank)
        rank = rank + leaves[-1].astype(jnp.int32)
    dests = {}
    for source in sorted({source + i for source, i in spans_of(groups, refs)}):
        peer = peer_of(me, half, source, False)
        dest = jnp.int32(-1)
        for j in range(reqs):
            hit = leaves[j] & (heard_ref[peer, 2 * reqs + j] == me)
            dest = jnp.where(hit, order[j], dest)
        dests[source] = dest
    parts, out_ref, bufs = refs[:count], refs[count + kept], refs[count + kept + 1 : -2]
    in_sems, out_sems = refs[-2:]
    steps = []
    for p, (source, origin) in enumerate(groups):
        base = pl.multiple_of(meta_ref[origin], ROWS)
        for i in range(parts[p].shape[0]):
            dest = dests[source + i]
            load = pltpu.make_async_copy(parts[p].at[i], bufs[p].at[i], in_sems.at[p, i])
            store = pltpu.make_async_copy(
                bufs[p].at[i],
                out_ref.at[jnp.maximum(dest, 0), pl.ds(base, parts[p].shape[1])],
                out_sems.at[p, i],
            )
            steps.append((dest >= 0, load, store))
    for used, load, store in steps:
        pl.when(used)(load.start)
    for used, load, store in steps:

        @pl.when(used)
        def _(load=load, store=store):
            load.wait()
            store.start()

    for used, load, store in steps:
        pl.when(used)(store.wait)


def spans_of(groups, parts):
    return [(source, i) for (source, _), part in zip(groups, parts) for i in range(part.shape[0])]


def place_parts(parts, groups, meta, heard, moves, shape, out=None):
    dtype = parts[0].dtype
    size = shape[0] * shape[1] * shape[2] * dtype.itemsize
    kept = [] if out is None else [out]
    most = max(part.shape[0] for part in parts)
    return pl.pallas_call(
        functools.partial(place_kernel, groups, len(kept), heard.shape[0] // 2),
        out_shape=jax.ShapeDtypeStruct(shape, dtype),
        in_specs=[SMEM] * 3 + [ANY] * (len(parts) + len(kept)),
        out_specs=ANY,
        input_output_aliases={3 + len(parts): 0} if kept else {},
        scratch_shapes=[pltpu.VMEM(part.shape, dtype) for part in parts]
        + [pltpu.SemaphoreType.DMA((len(parts), most))] * 2,
        cost_estimate=pl.CostEstimate(flops=size, bytes_accessed=size, transcendentals=0),
        name="place_parts",
    )(meta, heard, moves, *parts, *kept)


def attend(queries, keys_t, length, extra, extra_mask):
    scale = score_factor * log2_e
    near = jnp.dot(queries, keys_t, preferred_element_type=jnp.float32) * scale
    places = lax.broadcasted_iota(jnp.int32, (1, keys_t.shape[1]), 1)
    near = jnp.where(places < length, near, -jnp.inf)
    own = (
        lax.dot_general(
            queries, extra, (((1,), (1,)), ((), ())), preferred_element_type=jnp.float32
        )
        * scale
    )
    own = jnp.where(extra_mask, own, -jnp.inf)
    row_max = jnp.maximum(
        jnp.max(near, axis=1, keepdims=True), jnp.max(own, axis=1, keepdims=True)
    )
    near_weight = jnp.exp2(near - row_max)
    own_weight = jnp.exp2(own - row_max)
    total = jnp.sum(near_weight, axis=1, keepdims=True) + jnp.sum(
        own_weight, axis=1, keepdims=True
    )
    mixture = lax.dot_general(
        near_weight.astype(jnp.bfloat16),
        keys_t[:LAT],
        (((1,), (1,)), ((), ())),
        preferred_element_type=jnp.float32,
    )
    mixture = mixture + jnp.dot(
        own_weight.astype(jnp.bfloat16), extra[:, :LAT], preferred_element_type=jnp.float32
    )
    return (mixture * (1.0 / total)).astype(jnp.bfloat16)


def attend_kernel(groups, kept, half, meta_ref, heard_ref, first_ref, accept_ref, row_ref, *refs):
    parts = refs[: len(groups)]
    q1_ref, q2_ref, k1_ref, k2_ref = refs[len(groups) : len(groups) + 4]
    o1_ref, o2_ref, held, sems = refs[len(groups) + 4 + kept :]
    step = pl.program_id(0)
    me = meta_ref[0]
    base_slot = groups[0][0]

    @pl.when(step == 0)
    def _():
        used = {}
        for (request, origin), part in zip(groups, parts):
            base = pl.multiple_of(meta_ref[origin], ROWS)
            for i in range(part.shape[0]):
                slot = request + i - base_slot
                sem = used[slot] = used.get(slot, -1) + 1
                pltpu.make_async_copy(
                    part.at[i], held.at[slot, pl.ds(base, part.shape[1])], sems.at[slot, sem]
                ).start()

    request = row_ref[step]
    peer = first_ref[request]
    side = (peer // half == me // half).astype(jnp.int32)
    far = half + lax.rem(me + 2 * half - peer, half)
    slot = jnp.where(side == 1, lax.rem(peer, half), far) - base_slot
    for p in range(sems.shape[1]):
        rows = parts[0].shape[1]
        pltpu.make_async_copy(
            parts[0].at[0], held.at[slot, pl.ds(0, rows)], sems.at[slot, p]
        ).wait()

    rows = q1_ref.shape[1]
    reqs = first_ref.shape[0]
    draft = k1_ref.shape[0] // reqs
    heads = rows // draft
    keys = jnp.concatenate([k1_ref[...], k2_ref[...]], axis=0)
    row = lax.broadcasted_iota(jnp.int32, (rows, 1), 0)
    col = lax.broadcasted_iota(jnp.int32, (1, keys.shape[0]), 1)
    key = lax.div(col, reqs)
    own = lax.rem(col, reqs) == request
    first = own & (key < draft)
    causal = row >= lax.rem(key, draft) * heads
    taken = first & (key < accept_ref[request])
    keys_t = held[slot]
    length = heard_ref[peer, reqs + request]
    o1_ref[0] = attend(q1_ref[0], keys_t, length, keys, first & causal)
    o2_ref[0] = attend(
        q2_ref[0], keys_t, length, keys, taken | (own & (key >= draft) & causal)
    )


def attend_some(q1, q2, k1, k2, parts, groups, meta, heard, first, accepted, rows_of, outs=()):
    reqs, rows, width = q1.shape
    count = rows_of.shape[0]
    positions = parts[0].shape[2]
    each = sum(part.shape[0] for part in parts) // count
    block = lambda lanes: pl.BlockSpec((1, rows, lanes), lambda r, *refs: (refs[4][r], 0, 0))
    whole = pl.BlockSpec(k1.shape, lambda r, *_: (0, 0))
    out = jax.ShapeDtypeStruct((reqs, rows, LAT), jnp.bfloat16)
    flops = 2 * 2 * count * rows * positions * (width + LAT)
    start = 5 + len(parts) + 4
    return pl.pallas_call(
        functools.partial(attend_kernel, groups, len(outs), heard.shape[0] // 2),
        grid_spec=pltpu.PrefetchScalarGridSpec(
            num_scalar_prefetch=5,
            grid=(count,),
            in_specs=[ANY] * len(parts)
            + [block(width), block(width), whole, whole]
            + [ANY] * len(outs),
            out_specs=[block(LAT), block(LAT)],
            scratch_shapes=[
                pltpu.VMEM((count, width, positions), jnp.bfloat16),
                pltpu.SemaphoreType.DMA((count, each)),
            ],
        ),
        out_shape=(out, out),
        input_output_aliases={start + i: i for i in range(len(outs))},
        cost_estimate=pl.CostEstimate(
            flops=flops, bytes_accessed=count * width * positions * 4, transcendentals=0
        ),
        compiler_params=pltpu.CompilerParams(dimension_semantics=("arbitrary",)),
        name="attend_some",
    )(meta, heard, first, accepted, rows_of, *parts, q1, q2, k1, k2, *outs)


def program(
    queries_one,
    keys_one,
    queries_two,
    keys_two,
    latent_cache,
    cached_len,
    first_owner,
    new_owner,
    accepted,
):
    peers = lax.axis_size("cache")
    me = lax.axis_index("cache")
    groups = lax.axis_size("tok")
    group = lax.axis_index("tok")
    chips = groups // CORES
    reqs, draft, heads, width = queries_one.shape
    half = peers // 2
    halves = [[h * half + i for i in range(half)] for h in range(2)]

    def near_exchange(x):
        return lax.all_to_all(
            x, "cache", split_axis=0, concat_axis=0, tiled=True, axis_index_groups=halves
        )

    def far_shift(x, s):
        hop = [
            (h * half + i, (1 - h) * half + (i + s) % half) for h in range(2) for i in range(half)
        ]
        return lax.ppermute(x, "cache", hop)

    told = tell(first_owner, cached_len, new_owner, peers)
    heard = lax.all_to_all(told, "cache", split_axis=0, concat_axis=0, tiled=True)

    cache_t = jnp.swapaxes(latent_cache, 1, 2)
    share = round_up(-(-width // groups), ROWS)
    start_of = lambda t: jnp.minimum(t * share, width - share).astype(jnp.int32)
    chip, core = group // CORES, group % CORES
    origins = [group] + [(chip + chips - s) % chips * CORES + core for s in range(1, chips)]
    origins += [t + 1 - 2 * core for t in origins]
    wide = round_up(-(-width // CORES), ROWS)
    wide_of = lambda k: jnp.minimum(k * wide, width - wide).astype(jnp.int32)
    meta = jnp.stack(
        [me.astype(jnp.int32)]
        + [start_of(t) for t in origins]
        + [wide_of(core), wide_of(1 - core)]
    )
    swap = [(t, t + 1 - 2 * (t % CORES)) for t in range(groups)]

    def spread(part):
        held = [part]
        for s in range(1, chips):
            hop = [
                (c * CORES + k, (c + s) % chips * CORES + k)
                for c in range(chips)
                for k in range(CORES)
            ]
            held.append(lax.ppermute(part, "tok", hop))
        for x in held[:]:
            held.append(lax.ppermute(x, "tok", swap))
        return held

    plan = [(0, groups + 1)] + [(half + s, 1) for s in range(half)]
    sent = take_rows(
        cache_t, meta, new_owner, True, plan, [(half, wide)] + [(1, share)] * half
    )
    move_far = []
    for s in range(half):
        move_far.append(far_shift(sent[1 + s], s))
    move_near = near_exchange(sent[0])

    plan = [(0, 1)] + [(half + s, 1) for s in range(half)]
    sent = take_rows(cache_t, meta, heard, False, plan, [(half, share)] + [(1, share)] * half)
    draft_far = []
    for s in range(half):
        draft_far.append(far_shift(sent[1 + s], s))
    draft_near = near_exchange(sent[0])

    flat = (reqs, draft * heads, width)
    keys = (draft * reqs, width)
    operands = (
        queries_one.reshape(flat),
        queries_two.reshape(flat),
        jnp.swapaxes(keys_one, 0, 1).reshape(keys),
        jnp.swapaxes(keys_two, 0, 1).reshape(keys),
    )
    scalars = (meta, heard, first_owner, accepted)

    parts = spread(draft_near)
    where = [(0, 1 + k) for k in range(groups)]
    for s in range(half):
        parts += spread(draft_far[s])
        where += [(half + s, 1 + k) for k in range(groups)]
    rows_of = jnp.arange(reqs, dtype=jnp.int32)
    outs = attend_some(*operands, parts, where, *scalars, rows_of)

    tables = (meta, heard, new_owner)
    shape = (peers // 2, width, cache_t.shape[2])
    parts = [move_near, lax.ppermute(move_near, "tok", swap)]
    where = [(0, groups + 1), (0, groups + 2)]
    arrived = place_parts(parts, where, *tables, shape)
    parts, where = [], []
    for s in range(half):
        parts += spread(move_far[s])
        where += [(half + s, 1 + k) for k in range(groups)]
    arrived = place_parts(parts, where, *tables, shape, arrived)

    shape = (reqs, draft, heads, LAT)
    return outs[0].reshape(shape), outs[1].reshape(shape), jnp.swapaxes(arrived, 1, 2)


def solution(mesh):
    placed = (
        P("cache", None, "tok", None),
        P("cache", None, None),
        P("cache", None, "tok", None),
        P("cache", None, None),
        P("cache", None, None),
        P("cache"),
        P("cache"),
        P("cache"),
        P("cache"),
    )
    return jax.shard_map(
        program,
        mesh=mesh,
        in_specs=placed,
        out_specs=(
            P("cache", None, "tok", None),
            P("cache", None, "tok", None),
            P("cache", None, None),
        ),
        check_vma=False,
    )
```

```python
import functools

import jax
import jax.numpy as jnp
from jax import lax
from jax.experimental import pallas as pl
from jax.experimental.pallas import tpu as pltpu
from jax.sharding import PartitionSpec as P


LAT = 512
CORES = 2
ROWS = 16
LATE = 2

score_factor = 192.0 ** (-0.5)
log2_e = 1.4426950408889634
FREE = pl.BlockSpec(memory_space=pl.ANY)
ANY = pl.BlockSpec(memory_space=pl.ANY)
SMEM = pl.BlockSpec(memory_space=pltpu.SMEM)
VMEM = pl.BlockSpec(memory_space=pltpu.VMEM)


def round_up(value, step):
    return -(-value // step) * step


def tell_kernel(first_ref, length_ref, move_ref, out_ref):
    reqs = first_ref.shape[0]
    lane = lax.broadcasted_iota(jnp.int32, out_ref.shape, 1)
    row = jnp.zeros(out_ref.shape, jnp.int32)
    for t, ref in enumerate((first_ref, length_ref, move_ref)):
        for j in range(reqs):
            row = jnp.where(lane == t * reqs + j, ref[j], row)
    out_ref[...] = row


def tell(first_owner, cached_len, new_owner, peers):
    return pl.pallas_call(
        tell_kernel,
        out_shape=jax.ShapeDtypeStruct((peers, 3 * first_owner.shape[0]), jnp.int32),
        in_specs=[SMEM] * 3,
        out_specs=VMEM,
        name="tell",
    )(first_owner, cached_len, new_owner)


def peer_of(me, half, s, to):
    side, place = me // half, me % half
    if s < half:
        return side * half + s
    shift = s - half if to else 2 * half - s
    return (1 - side) * half + lax.rem(place + shift, half)


def take_kernel(plan, half, moves, meta_ref, slots_ref, table_ref, *refs):
    outs, sems = refs[: len(plan)], refs[-1]
    me = meta_ref[0]
    for p, rows_ref in enumerate(refs[len(plan) : -1]):
        for i in range(half):
            peer = peer_of(me, half, p * half + i, False)
            row = jnp.int32(0)
            for j in range(2 * half):
                row = jnp.where(slots_ref[me, j] == peer, j, row)
            rows_ref[i] = row
    copies = []
    for out_ref, (first, part) in zip(outs, plan):
        base = pl.multiple_of(meta_ref[part], ROWS)
        for d in range(out_ref.shape[0]):
            peer = peer_of(me, half, first + d, True)
            slot = jnp.int32(0)
            for j in range(2 * half):
                if moves:
                    hit = (slots_ref[j] == peer) & (peer != me)
                else:
                    hit = slots_ref[peer, j] == me
                slot = jnp.where(hit, j, slot)
            copies.append(
                pltpu.make_async_copy(
                    table_ref.at[slot, pl.ds(base, out_ref.shape[1])],
                    out_ref.at[d],
                    sems.at[first + d],
                )
            )
    for copy in copies:
        copy.start()
    for copy in copies:
        copy.wait()


def take_rows(table, meta, slots, moves, plan, shapes):
    lanes = table.shape[2]
    count = sum(shape[0] for shape in shapes)
    lists = 0 if moves else 2
    size = sum(n * rows for n, rows in shapes) * lanes * table.dtype.itemsize
    return pl.pallas_call(
        functools.partial(take_kernel, plan, count // 2, moves),
        out_shape=[jax.ShapeDtypeStruct(shape + (lanes,), table.dtype) for shape in shapes]
        + [jax.ShapeDtypeStruct((count // 2,), jnp.int32)] * lists,
        in_specs=[SMEM, SMEM, ANY],
        out_specs=[VMEM] * len(shapes) + [SMEM] * lists,
        scratch_shapes=[pltpu.SemaphoreType.DMA((count,))],
        cost_estimate=pl.CostEstimate(flops=2 * size, bytes_accessed=2 * size, transcendentals=0),
        name="take_rows",
    )(meta, slots, table)


def place_kernel(groups, kept, half, meta_ref, heard_ref, move_ref, *refs):
    count = len(groups)
    reqs = move_ref.shape[0]
    me = meta_ref[0]
    order, leaves = [], []
    rank = jnp.int32(0)
    for j in range(reqs):
        leaves.append(move_ref[j] != me)
        order.append(rank)
        rank = rank + leaves[-1].astype(jnp.int32)
    dests = {}
    for source in sorted({source + i for source, i in spans_of(groups, refs)}):
        peer = peer_of(me, half, source, False)
        dest = jnp.int32(-1)
        for j in range(reqs):
            hit = leaves[j] & (heard_ref[peer, 2 * reqs + j] == me)
            dest = jnp.where(hit, order[j], dest)
        dests[source] = dest
    parts, out_ref, bufs = refs[:count], refs[count + kept], refs[count + kept + 1 : -2]
    in_sems, out_sems = refs[-2:]
    steps = []
    for p, (source, origin) in enumerate(groups):
        base = pl.multiple_of(meta_ref[origin], ROWS)
        for i in range(parts[p].shape[0]):
            dest = dests[source + i]
            load = pltpu.make_async_copy(parts[p].at[i], bufs[p].at[i], in_sems.at[p, i])
            store = pltpu.make_async_copy(
                bufs[p].at[i],
                out_ref.at[jnp.maximum(dest, 0), pl.ds(base, parts[p].shape[1])],
                out_sems.at[p, i],
            )
            steps.append((dest >= 0, load, store))
    for used, load, store in steps:
        pl.when(used)(load.start)
    for used, load, store in steps:

        @pl.when(used)
        def _(load=load, store=store):
            load.wait()
            store.start()

    for used, load, store in steps:
        pl.when(used)(store.wait)


def spans_of(groups, parts):
    return [(source, i) for (source, _), part in zip(groups, parts) for i in range(part.shape[0])]


def place_parts(parts, groups, meta, heard, moves, shape, out=None):
    dtype = parts[0].dtype
    size = shape[0] * shape[1] * shape[2] * dtype.itemsize
    kept = [] if out is None else [out]
    most = max(part.shape[0] for part in parts)
    return pl.pallas_call(
        functools.partial(place_kernel, groups, len(kept), heard.shape[0] // 2),
        out_shape=jax.ShapeDtypeStruct(shape, dtype),
        in_specs=[SMEM] * 3 + [FREE] * (len(parts) + len(kept)),
        out_specs=ANY,
        input_output_aliases={3 + len(parts): 0} if kept else {},
        scratch_shapes=[pltpu.VMEM(part.shape, dtype) for part in parts]
        + [pltpu.SemaphoreType.DMA((len(parts), most))] * 2,
        cost_estimate=pl.CostEstimate(flops=size, bytes_accessed=size, transcendentals=0),
        name="place_parts",
    )(meta, heard, moves, *parts, *kept)


def attend(queries, keys_t, length, extra, extra_mask):
    scale = score_factor * log2_e
    near = jnp.dot(queries, keys_t, preferred_element_type=jnp.float32) * scale
    places = lax.broadcasted_iota(jnp.int32, (1, keys_t.shape[1]), 1)
    near = jnp.where(places < length, near, -jnp.inf)
    own = (
        lax.dot_general(
            queries, extra, (((1,), (1,)), ((), ())), preferred_element_type=jnp.float32
        )
        * scale
    )
    own = jnp.where(extra_mask, own, -jnp.inf)
    row_max = jnp.maximum(
        jnp.max(near, axis=1, keepdims=True), jnp.max(own, axis=1, keepdims=True)
    )
    near_weight = jnp.exp2(near - row_max)
    own_weight = jnp.exp2(own - row_max)
    total = jnp.sum(near_weight, axis=1, keepdims=True) + jnp.sum(
        own_weight, axis=1, keepdims=True
    )
    mixture = lax.dot_general(
        near_weight.astype(jnp.bfloat16),
        keys_t[:LAT],
        (((1,), (1,)), ((), ())),
        preferred_element_type=jnp.float32,
    )
    mixture = mixture + jnp.dot(
        own_weight.astype(jnp.bfloat16), extra[:, :LAT], preferred_element_type=jnp.float32
    )
    return (mixture * (1.0 / total)).astype(jnp.bfloat16)


def attend_kernel(groups, kept, meta_ref, heard_ref, first_ref, accept_ref, row_ref, *refs):
    parts = refs[: len(groups)]
    q1_hbm, q2_hbm, k1_ref, k2_ref = refs[len(groups) : len(groups) + 4]
    o1_ref, o2_ref, held, q1_held, q2_held, sems, q_sems = refs[len(groups) + 4 + kept :]
    step = pl.program_id(0)
    base_slot = groups[0][0]

    def query_copies(index):
        for k, (src, dst) in enumerate(((q1_hbm, q1_held), (q2_hbm, q2_held))):
            yield pltpu.make_async_copy(src.at[row_ref[index]], dst.at[index], q_sems.at[index, k])

    @pl.when(step == 0)
    def _():
        used = {}
        loads = []
        for (request, origin), part in zip(groups, parts):
            base = pl.multiple_of(meta_ref[origin], ROWS)
            for i in range(part.shape[0]):
                slot = request + i - base_slot
                sem = used[slot] = used.get(slot, -1) + 1
                copy = pltpu.make_async_copy(
                    part.at[i], held.at[slot, pl.ds(base, part.shape[1])], sems.at[slot, sem]
                )
                loads.append((slot, copy))
        loads.sort(key=lambda load: load[0])
        for index in range(held.shape[0]):
            for copy in query_copies(index):
                copy.start()
            for slot, copy in loads:
                if slot == index:
                    copy.start()

    for copy in query_copies(step):
        copy.wait()
    request = row_ref[step]
    peer = first_ref[request]
    for p in range(sems.shape[1]):
        rows = parts[0].shape[1]
        pltpu.make_async_copy(
            parts[0].at[0], held.at[step, pl.ds(0, rows)], sems.at[step, p]
        ).wait()

    rows = q1_held.shape[1]
    reqs = first_ref.shape[0]
    draft = k1_ref.shape[0] // reqs
    heads = rows // draft
    keys = jnp.concatenate([k1_ref[...], k2_ref[...]], axis=0)
    row = lax.broadcasted_iota(jnp.int32, (2 * rows, 1), 0)
    col = lax.broadcasted_iota(jnp.int32, (1, keys.shape[0]), 1)
    key = lax.div(col, reqs)
    own = lax.rem(col, reqs) == request
    first = own & (key < draft)
    second = row >= rows
    causal = row - jnp.where(second, rows, 0) >= lax.rem(key, draft) * heads
    taken = first & (key < accept_ref[request])
    mask = (first & causal & ~second) | (
        (taken | (own & (key >= draft) & causal)) & second
    )
    keys_t = held[step]
    length = heard_ref[peer, reqs + request]
    queries = jnp.concatenate([q1_held[step], q2_held[step]], axis=0)
    out = attend(queries, keys_t, length, keys, mask)
    o1_ref[0] = out[:rows]
    o2_ref[0] = out[rows:]


def attend_some(q1, q2, k1, k2, parts, groups, meta, heard, first, accepted, rows_of, outs=()):
    reqs, rows, width = q1.shape
    count = rows_of.shape[0]
    positions = parts[0].shape[2]
    each = sum(part.shape[0] for part in parts) // count
    block = lambda lanes: pl.BlockSpec((1, rows, lanes), lambda r, *refs: (refs[4][r], 0, 0))
    whole = pl.BlockSpec(k1.shape, lambda r, *_: (0, 0))
    out = jax.ShapeDtypeStruct((reqs, rows, LAT), jnp.bfloat16)
    flops = 2 * 2 * count * rows * positions * (width + LAT)
    start = 5 + len(parts) + 4
    return pl.pallas_call(
        functools.partial(attend_kernel, groups, len(outs)),
        grid_spec=pltpu.PrefetchScalarGridSpec(
            num_scalar_prefetch=5,
            grid=(count,),
            in_specs=[ANY] * len(parts)
            + [ANY, ANY, whole, whole]
            + [ANY] * len(outs),
            out_specs=[block(LAT), block(LAT)],
            scratch_shapes=[
                pltpu.VMEM((count, width, positions), jnp.bfloat16),
                pltpu.VMEM((count, rows, width), jnp.bfloat16),
                pltpu.VMEM((count, rows, width), jnp.bfloat16),
                pltpu.SemaphoreType.DMA((count, each)),
                pltpu.SemaphoreType.DMA((count, 2)),
            ],
        ),
        out_shape=(out, out),
        input_output_aliases={start + i: i for i in range(len(outs))},
        cost_estimate=pl.CostEstimate(
            flops=flops, bytes_accessed=count * width * positions * 4, transcendentals=0
        ),
        compiler_params=pltpu.CompilerParams(dimension_semantics=("arbitrary",)),
        name="attend_some",
    )(meta, heard, first, accepted, rows_of, *parts, q1, q2, k1, k2, *outs)


def program(
    queries_one,
    keys_one,
    queries_two,
    keys_two,
    latent_cache,
    cached_len,
    first_owner,
    new_owner,
    accepted,
):
    peers = lax.axis_size("cache")
    me = lax.axis_index("cache")
    groups = lax.axis_size("tok")
    group = lax.axis_index("tok")
    chips = groups // CORES
    reqs, draft, heads, width = queries_one.shape
    half = peers // 2
    halves = [[h * half + i for i in range(half)] for h in range(2)]

    def near_exchange(x):
        return lax.all_to_all(
            x, "cache", split_axis=0, concat_axis=0, tiled=True, axis_index_groups=halves
        )

    def far_shift(x, s):
        hop = [
            (h * half + i, (1 - h) * half + (i + s) % half) for h in range(2) for i in range(half)
        ]
        return lax.ppermute(x, "cache", hop)

    told = tell(first_owner, cached_len, new_owner, peers)
    heard = lax.all_to_all(told, "cache", split_axis=0, concat_axis=0, tiled=True)

    cache_t = jnp.swapaxes(latent_cache, 1, 2)
    share = round_up(-(-width // groups), ROWS)
    start_of = lambda t: jnp.minimum(t * share, width - share).astype(jnp.int32)
    chip, core = group // CORES, group % CORES
    origins = [group] + [(chip + chips - s) % chips * CORES + core for s in range(1, chips)]
    origins += [t + 1 - 2 * core for t in origins]
    wide = round_up(-(-width // CORES), ROWS)
    wide_of = lambda k: jnp.minimum(k * wide, width - wide).astype(jnp.int32)
    meta = jnp.stack(
        [me.astype(jnp.int32)]
        + [start_of(t) for t in origins]
        + [wide_of(core), wide_of(1 - core)]
    )
    swap = [(t, t + 1 - 2 * (t % CORES)) for t in range(groups)]

    def spread(part):
        held = [part]
        for s in range(1, chips):
            hop = [
                (c * CORES + k, (c + s) % chips * CORES + k)
                for c in range(chips)
                for k in range(CORES)
            ]
            held.append(lax.ppermute(part, "tok", hop))
        for x in held[:]:
            held.append(lax.ppermute(x, "tok", swap))
        return held

    plan = [(0, groups + 1)] + [(half + s, 1) for s in range(half)]
    sent = take_rows(
        cache_t, meta, new_owner, True, plan, [(half, wide)] + [(1, share)] * half
    )
    move_far = []
    for s in range(half):
        move_far.append(far_shift(sent[1 + s], s))
    move_near = near_exchange(sent[0])

    plan = [(0, 1)] + [(half + s, 1) for s in range(half)]
    *sent, rows_near, rows_far = take_rows(
        cache_t, meta, heard, False, plan, [(half, share)] + [(1, share)] * half
    )
    draft_far = []
    for s in range(half):
        draft_far.append(far_shift(sent[1 + s], s))
    draft_near = near_exchange(sent[0])

    flat = (reqs, draft * heads, width)
    keys = (draft * reqs, width)
    operands = (
        queries_one.reshape(flat),
        queries_two.reshape(flat),
        jnp.swapaxes(keys_one, 0, 1).reshape(keys),
        jnp.swapaxes(keys_two, 0, 1).reshape(keys),
    )
    scalars = (meta, heard, first_owner, accepted)

    parts = spread(draft_near)
    where = [(0, 1 + k) for k in range(groups)]
    outs = attend_some(*operands, parts, where, *scalars, rows_near)
    parts, where = [], []
    for s in range(half):
        parts += spread(draft_far[s])
        where += [(half + s, 1 + k) for k in range(groups)]
    outs = attend_some(*operands, parts, where, *scalars, rows_far, outs)

    tables = (meta, heard, new_owner)
    shape = (peers // 2, width, cache_t.shape[2])
    parts = [move_near, lax.ppermute(move_near, "tok", swap)]
    where = [(0, groups + 1), (0, groups + 2)]
    early = half - LATE
    for s in range(half):
        if s == early:
            arrived = place_parts(parts, where, *tables, shape)
            parts, where = [], []
        parts += spread(move_far[s])
        where += [(half + s, 1 + k) for k in range(groups)]
    arrived = place_parts(parts, where, *tables, shape, arrived)

    shape = (reqs, draft, heads, LAT)
    return outs[0].reshape(shape), outs[1].reshape(shape), jnp.swapaxes(arrived, 1, 2)


def solution(mesh):
    placed = (
        P("cache", None, "tok", None),
        P("cache", None, None),
        P("cache", None, "tok", None),
        P("cache", None, None),
        P("cache", None, None),
        P("cache"),
        P("cache"),
        P("cache"),
        P("cache"),
    )
    return jax.shard_map(
        program,
        mesh=mesh,
        in_specs=placed,
        out_specs=(
            P("cache", None, "tok", None),
            P("cache", None, "tok", None),
            P("cache", None, None),
        ),
        check_vma=False,
    )
```

```python
import functools

import jax
import jax.numpy as jnp
from jax import lax
from jax.experimental import pallas as pl
from jax.experimental.pallas import tpu as pltpu
from jax.sharding import PartitionSpec as P


LAT = 512
CORES = 2
ROWS = 16
LATE = 3

score_factor = 192.0 ** (-0.5)
log2_e = 1.4426950408889634
FREE = pl.BlockSpec(memory_space=pl.ANY)
ANY = pl.BlockSpec(memory_space=pl.ANY)
SMEM = pl.BlockSpec(memory_space=pltpu.SMEM)
VMEM = pl.BlockSpec(memory_space=pltpu.VMEM)


def round_up(value, step):
    return -(-value // step) * step


def tell_kernel(first_ref, length_ref, move_ref, out_ref):
    reqs = first_ref.shape[0]
    lane = lax.broadcasted_iota(jnp.int32, out_ref.shape, 1)
    row = jnp.zeros(out_ref.shape, jnp.int32)
    for t, ref in enumerate((first_ref, length_ref, move_ref)):
        for j in range(reqs):
            row = jnp.where(lane == t * reqs + j, ref[j], row)
    out_ref[...] = row


def tell(first_owner, cached_len, new_owner, peers):
    return pl.pallas_call(
        tell_kernel,
        out_shape=jax.ShapeDtypeStruct((peers, 3 * first_owner.shape[0]), jnp.int32),
        in_specs=[SMEM] * 3,
        out_specs=VMEM,
        name="tell",
    )(first_owner, cached_len, new_owner)


def peer_of(me, half, s, to):
    side, place = me // half, me % half
    if s < half:
        return side * half + s
    shift = s - half if to else 2 * half - s
    return (1 - side) * half + lax.rem(place + shift, half)


def take_kernel(plan, half, moves, meta_ref, slots_ref, table_ref, *refs):
    outs, sems = refs[: len(plan)], refs[-1]
    me = meta_ref[0]
    for p, rows_ref in enumerate(refs[len(plan) : -1]):
        for i in range(half):
            peer = peer_of(me, half, p * half + i, False)
            row = jnp.int32(0)
            for j in range(2 * half):
                row = jnp.where(slots_ref[me, j] == peer, j, row)
            rows_ref[i] = row
    copies = []
    for out_ref, (first, part) in zip(outs, plan):
        base = pl.multiple_of(meta_ref[part], ROWS)
        for d in range(out_ref.shape[0]):
            peer = peer_of(me, half, first + d, True)
            slot = jnp.int32(0)
            for j in range(2 * half):
                if moves:
                    hit = (slots_ref[j] == peer) & (peer != me)
                else:
                    hit = slots_ref[peer, j] == me
                slot = jnp.where(hit, j, slot)
            copies.append(
                pltpu.make_async_copy(
                    table_ref.at[slot, pl.ds(base, out_ref.shape[1])],
                    out_ref.at[d],
                    sems.at[first + d],
                )
            )
    for copy in copies:
        copy.start()
    for copy in copies:
        copy.wait()


def take_rows(table, meta, slots, moves, plan, shapes):
    lanes = table.shape[2]
    count = sum(shape[0] for shape in shapes)
    lists = 0 if moves else 2
    size = sum(n * rows for n, rows in shapes) * lanes * table.dtype.itemsize
    return pl.pallas_call(
        functools.partial(take_kernel, plan, count // 2, moves),
        out_shape=[jax.ShapeDtypeStruct(shape + (lanes,), table.dtype) for shape in shapes]
        + [jax.ShapeDtypeStruct((count // 2,), jnp.int32)] * lists,
        in_specs=[SMEM, SMEM, ANY],
        out_specs=[VMEM] * len(shapes) + [SMEM] * lists,
        scratch_shapes=[pltpu.SemaphoreType.DMA((count,))],
        cost_estimate=pl.CostEstimate(flops=2 * size, bytes_accessed=2 * size, transcendentals=0),
        name="take_rows",
    )(meta, slots, table)


def place_kernel(groups, kept, half, meta_ref, heard_ref, move_ref, *refs):
    count = len(groups)
    reqs = move_ref.shape[0]
    me = meta_ref[0]
    order, leaves = [], []
    rank = jnp.int32(0)
    for j in range(reqs):
        leaves.append(move_ref[j] != me)
        order.append(rank)
        rank = rank + leaves[-1].astype(jnp.int32)
    dests = {}
    for source in sorted({source + i for source, i in spans_of(groups, refs)}):
        peer = peer_of(me, half, source, False)
        dest = jnp.int32(-1)
        for j in range(reqs):
            hit = leaves[j] & (heard_ref[peer, 2 * reqs + j] == me)
            dest = jnp.where(hit, order[j], dest)
        dests[source] = dest
    parts, out_ref, bufs = refs[:count], refs[count + kept], refs[count + kept + 1 : -2]
    in_sems, out_sems = refs[-2:]
    steps = []
    for p, (source, origin) in enumerate(groups):
        base = pl.multiple_of(meta_ref[origin], ROWS)
        for i in range(parts[p].shape[0]):
            dest = dests[source + i]
            load = pltpu.make_async_copy(parts[p].at[i], bufs[p].at[i], in_sems.at[p, i])
            store = pltpu.make_async_copy(
                bufs[p].at[i],
                out_ref.at[jnp.maximum(dest, 0), pl.ds(base, parts[p].shape[1])],
                out_sems.at[p, i],
            )
            steps.append((dest >= 0, load, store))
    for used, load, store in steps:
        pl.when(used)(load.start)
    for used, load, store in steps:

        @pl.when(used)
        def _(load=load, store=store):
            load.wait()
            store.start()

    for used, load, store in steps:
        pl.when(used)(store.wait)


def spans_of(groups, parts):
    return [(source, i) for (source, _), part in zip(groups, parts) for i in range(part.shape[0])]


def place_parts(parts, groups, meta, heard, moves, shape, out=None):
    dtype = parts[0].dtype
    size = shape[0] * shape[1] * shape[2] * dtype.itemsize
    kept = [] if out is None else [out]
    most = max(part.shape[0] for part in parts)
    return pl.pallas_call(
        functools.partial(place_kernel, groups, len(kept), heard.shape[0] // 2),
        out_shape=jax.ShapeDtypeStruct(shape, dtype),
        in_specs=[SMEM] * 3 + [FREE] * (len(parts) + len(kept)),
        out_specs=ANY,
        input_output_aliases={3 + len(parts): 0} if kept else {},
        scratch_shapes=[pltpu.VMEM(part.shape, dtype) for part in parts]
        + [pltpu.SemaphoreType.DMA((len(parts), most))] * 2,
        cost_estimate=pl.CostEstimate(flops=size, bytes_accessed=size, transcendentals=0),
        name="place_parts",
    )(meta, heard, moves, *parts, *kept)


def attend(queries, keys_t, length, extra, extra_mask):
    scale = score_factor * log2_e
    near = jnp.dot(queries, keys_t, preferred_element_type=jnp.float32) * scale
    places = lax.broadcasted_iota(jnp.int32, (1, keys_t.shape[1]), 1)
    near = jnp.where(places < length, near, -jnp.inf)
    own = (
        lax.dot_general(
            queries, extra, (((1,), (1,)), ((), ())), preferred_element_type=jnp.float32
        )
        * scale
    )
    own = jnp.where(extra_mask, own, -jnp.inf)
    row_max = jnp.maximum(
        jnp.max(near, axis=1, keepdims=True), jnp.max(own, axis=1, keepdims=True)
    )
    near_weight = jnp.exp2(near - row_max)
    own_weight = jnp.exp2(own - row_max)
    total = jnp.sum(near_weight, axis=1, keepdims=True) + jnp.sum(
        own_weight, axis=1, keepdims=True
    )
    mixture = lax.dot_general(
        near_weight.astype(jnp.bfloat16),
        keys_t[:LAT],
        (((1,), (1,)), ((), ())),
        preferred_element_type=jnp.float32,
    )
    mixture = mixture + jnp.dot(
        own_weight.astype(jnp.bfloat16), extra[:, :LAT], preferred_element_type=jnp.float32
    )
    return (mixture * (1.0 / total)).astype(jnp.bfloat16)


def attend_kernel(groups, kept, meta_ref, heard_ref, first_ref, accept_ref, row_ref, *refs):
    parts = refs[: len(groups)]
    q1_hbm, q2_hbm, *keys_hbm = refs[len(groups) : len(groups) + 4]
    o1_ref, o2_ref, held, q1_held, q2_held, keys_ref, sems, q_sems, k_sems = refs[
        len(groups) + 4 + kept :
    ]
    own_keys = keys_ref.shape[0] // 2
    key_copies = [
        pltpu.make_async_copy(src, keys_ref.at[pl.ds(k * own_keys, own_keys)], k_sems.at[k])
        for k, src in enumerate(keys_hbm)
    ]
    step = pl.program_id(0)
    base_slot = groups[0][0]

    def query_copies(index):
        for k, (src, dst) in enumerate(((q1_hbm, q1_held), (q2_hbm, q2_held))):
            yield pltpu.make_async_copy(src.at[row_ref[index]], dst.at[index], q_sems.at[index, k])

    @pl.when(step == 0)
    def _():
        used = {}
        loads = []
        for (request, origin), part in zip(groups, parts):
            base = pl.multiple_of(meta_ref[origin], ROWS)
            for i in range(part.shape[0]):
                slot = request + i - base_slot
                sem = used[slot] = used.get(slot, -1) + 1
                copy = pltpu.make_async_copy(
                    part.at[i], held.at[slot, pl.ds(base, part.shape[1])], sems.at[slot, sem]
                )
                loads.append((slot, copy))
        loads.sort(key=lambda load: load[0])
        for copy in key_copies:
            copy.start()
        for index in range(held.shape[0]):
            for copy in query_copies(index):
                copy.start()
            for slot, copy in loads:
                if slot == index:
                    copy.start()

        for copy in key_copies:
            copy.wait()

    for copy in query_copies(step):
        copy.wait()
    request = row_ref[step]
    peer = first_ref[request]
    for p in range(sems.shape[1]):
        rows = parts[0].shape[1]
        pltpu.make_async_copy(
            parts[0].at[0], held.at[step, pl.ds(0, rows)], sems.at[step, p]
        ).wait()

    rows = q1_held.shape[1]
    reqs = first_ref.shape[0]
    draft = own_keys // reqs
    heads = rows // draft
    keys = keys_ref[...]
    row = lax.broadcasted_iota(jnp.int32, (2 * rows, 1), 0)
    col = lax.broadcasted_iota(jnp.int32, (1, keys.shape[0]), 1)
    key = lax.div(col, reqs)
    own = lax.rem(col, reqs) == request
    first = own & (key < draft)
    second = row >= rows
    causal = row - jnp.where(second, rows, 0) >= lax.rem(key, draft) * heads
    taken = first & (key < accept_ref[request])
    mask = (first & causal & ~second) | (
        (taken | (own & (key >= draft) & causal)) & second
    )
    keys_t = held[step]
    length = heard_ref[peer, reqs + request]
    queries = jnp.concatenate([q1_held[step], q2_held[step]], axis=0)
    out = attend(queries, keys_t, length, keys, mask)
    o1_ref[0] = out[:rows]
    o2_ref[0] = out[rows:]


def attend_some(q1, q2, k1, k2, parts, groups, meta, heard, first, accepted, rows_of, outs=()):
    reqs, rows, width = q1.shape
    count = rows_of.shape[0]
    positions = parts[0].shape[2]
    each = sum(part.shape[0] for part in parts) // count
    block = lambda lanes: pl.BlockSpec((1, rows, lanes), lambda r, *refs: (refs[4][r], 0, 0))
    out = jax.ShapeDtypeStruct((reqs, rows, LAT), jnp.bfloat16)
    flops = 2 * 2 * count * rows * positions * (width + LAT)
    start = 5 + len(parts) + 4
    return pl.pallas_call(
        functools.partial(attend_kernel, groups, len(outs)),
        grid_spec=pltpu.PrefetchScalarGridSpec(
            num_scalar_prefetch=5,
            grid=(count,),
            in_specs=[ANY] * len(parts)
            + [ANY] * 4
            + [ANY] * len(outs),
            out_specs=[block(LAT), block(LAT)],
            scratch_shapes=[
                pltpu.VMEM((count, width, positions), jnp.bfloat16),
                pltpu.VMEM((count, rows, width), jnp.bfloat16),
                pltpu.VMEM((count, rows, width), jnp.bfloat16),
                pltpu.VMEM((2 * k1.shape[0], width), jnp.bfloat16),
                pltpu.SemaphoreType.DMA((count, each)),
                pltpu.SemaphoreType.DMA((count, 2)),
                pltpu.SemaphoreType.DMA((2,)),
            ],
        ),
        out_shape=(out, out),
        input_output_aliases={start + i: i for i in range(len(outs))},
        cost_estimate=pl.CostEstimate(
            flops=flops, bytes_accessed=count * width * positions * 4, transcendentals=0
        ),
        compiler_params=pltpu.CompilerParams(dimension_semantics=("arbitrary",)),
        name="attend_some",
    )(meta, heard, first, accepted, rows_of, *parts, q1, q2, k1, k2, *outs)


def program(
    queries_one,
    keys_one,
    queries_two,
    keys_two,
    latent_cache,
    cached_len,
    first_owner,
    new_owner,
    accepted,
):
    peers = lax.axis_size("cache")
    me = lax.axis_index("cache")
    groups = lax.axis_size("tok")
    group = lax.axis_index("tok")
    chips = groups // CORES
    reqs, draft, heads, width = queries_one.shape
    half = peers // 2
    halves = [[h * half + i for i in range(half)] for h in range(2)]

    def near_exchange(x):
        return lax.all_to_all(
            x, "cache", split_axis=0, concat_axis=0, tiled=True, axis_index_groups=halves
        )

    def far_shift(x, s):
        hop = [
            (h * half + i, (1 - h) * half + (i + s) % half) for h in range(2) for i in range(half)
        ]
        return lax.ppermute(x, "cache", hop)

    told = tell(first_owner, cached_len, new_owner, peers)
    heard = lax.all_to_all(told, "cache", split_axis=0, concat_axis=0, tiled=True)

    cache_t = jnp.swapaxes(latent_cache, 1, 2)
    share = round_up(-(-width // groups), ROWS)
    start_of = lambda t: jnp.minimum(t * share, width - share).astype(jnp.int32)
    chip, core = group // CORES, group % CORES
    origins = [group] + [(chip + chips - s) % chips * CORES + core for s in range(1, chips)]
    origins += [t + 1 - 2 * core for t in origins]
    wide = round_up(-(-width // CORES), ROWS)
    wide_of = lambda k: jnp.minimum(k * wide, width - wide).astype(jnp.int32)
    meta = jnp.stack(
        [me.astype(jnp.int32)]
        + [start_of(t) for t in origins]
        + [wide_of(core), wide_of(1 - core)]
    )
    swap = [(t, t + 1 - 2 * (t % CORES)) for t in range(groups)]

    def spread(part):
        held = [part]
        for s in range(1, chips):
            hop = [
                (c * CORES + k, (c + s) % chips * CORES + k)
                for c in range(chips)
                for k in range(CORES)
            ]
            held.append(lax.ppermute(part, "tok", hop))
        for x in held[:]:
            held.append(lax.ppermute(x, "tok", swap))
        return held

    plan = [(0, groups + 1)] + [(half + s, 1) for s in range(half)]
    sent = take_rows(
        cache_t, meta, new_owner, True, plan, [(half, wide)] + [(1, share)] * half
    )
    move_far = []
    for s in range(half):
        move_far.append(far_shift(sent[1 + s], s))
    move_near = near_exchange(sent[0])

    plan = [(0, 1)] + [(half + s, 1) for s in range(half)]
    *sent, rows_near, rows_far = take_rows(
        cache_t, meta, heard, False, plan, [(half, share)] + [(1, share)] * half
    )
    draft_far = []
    for s in range(half):
        draft_far.append(far_shift(sent[1 + s], s))
    draft_near = near_exchange(sent[0])

    flat = (reqs, draft * heads, width)
    keys = (draft * reqs, width)
    operands = (
        queries_one.reshape(flat),
        queries_two.reshape(flat),
        jnp.swapaxes(keys_one, 0, 1).reshape(keys),
        jnp.swapaxes(keys_two, 0, 1).reshape(keys),
    )
    scalars = (meta, heard, first_owner, accepted)

    parts = spread(draft_near)
    where = [(0, 1 + k) for k in range(groups)]
    outs = attend_some(*operands, parts, where, *scalars, rows_near)
    parts, where = [], []
    for s in range(half):
        parts += spread(draft_far[s])
        where += [(half + s, 1 + k) for k in range(groups)]
    outs = attend_some(*operands, parts, where, *scalars, rows_far, outs)

    tables = (meta, heard, new_owner)
    shape = (peers // 2, width, cache_t.shape[2])
    parts = [move_near, lax.ppermute(move_near, "tok", swap)]
    where = [(0, groups + 1), (0, groups + 2)]
    early = half - LATE
    for s in range(half):
        if s == early:
            arrived = place_parts(parts, where, *tables, shape)
            parts, where = [], []
        parts += spread(move_far[s])
        where += [(half + s, 1 + k) for k in range(groups)]
    arrived = place_parts(parts, where, *tables, shape, arrived)

    shape = (reqs, draft, heads, LAT)
    return outs[0].reshape(shape), outs[1].reshape(shape), jnp.swapaxes(arrived, 1, 2)


def solution(mesh):
    placed = (
        P("cache", None, "tok", None),
        P("cache", None, None),
        P("cache", None, "tok", None),
        P("cache", None, None),
        P("cache", None, None),
        P("cache"),
        P("cache"),
        P("cache"),
        P("cache"),
    )
    return jax.shard_map(
        program,
        mesh=mesh,
        in_specs=placed,
        out_specs=(
            P("cache", None, "tok", None),
            P("cache", None, "tok", None),
            P("cache", None, None),
        ),
        check_vma=False,
    )
```
